32 devices in a mesh: rep: 1 (over z), data: 4 (over y), table: 8 (over x, core).
Axes of the slice: x: 4, y: 4, z: 1, core: 2. Of those that a mesh axis runs over, the one named last changes fastest.
The devices are a block of a 4x4x8 slice.
Arguments:
- tokens: bfloat16 [8192, 1024], P(('rep', 'data', 'table'))
- table_u: bfloat16 [65536, 1024], P(('rep', 'table'))
- table_v: bfloat16 [65536, 1024], P(('rep', 'table'))
- expert_ids: int32 [8192, 8, 16], P(('rep', 'data', 'table'))
- gate_vals: float32 [8192, 8, 16], P(('rep', 'data', 'table'))
- grad_out: bfloat16 [8192, 1024], P(('rep', 'data', 'table'))
Outputs:
- output 1: bfloat16 [8192, 1024], P(('rep', 'data', 'table'))
- output 2: bfloat16 [8192, 1024], P(('rep', 'data', 'table'))
- output 3: bfloat16 [65536, 1024], P(('rep', 'table', 'data'))
- output 4: bfloat16 [65536, 1024], P(('rep', 'table', 'data'))
All inputs are finite; a program needn't handle non-finite values.
Results may differ from the reference program's by a relative error of at most 0.001.
Values are sent between devices in bfloat16 or wider.
A program may use at most 768 MiB of HBM per device.

```python
import jax
import jax.numpy as jnp
from jax import lax

DIM_MODEL = 1024
EXPERTS = 65536
N_HEADS = 8
TOP_K = 16
TOK_DEV = 256
DATA_DEVS = 4
TABLE_DEVS = 8

SEL_TOK = N_HEADS * TOP_K
N_DEVS = DATA_DEVS * TABLE_DEVS
PART_TOKENS = N_DEVS * TOK_DEV
BLOCK_ROWS = EXPERTS // TABLE_DEVS
POOL_ROWS = TOK_DEV * SEL_TOK // (4 * TABLE_DEVS)
SEL_DEV = TOK_DEV * SEL_TOK
COVERED = TABLE_DEVS * POOL_ROWS


def one_device(dev_key, dev_pool):
    k_order, k_own_a, k_own_b, k_ent_a, k_ent_b = jax.random.split(dev_key, 5)
    sel_order = jax.random.permutation(k_order, SEL_DEV)
    owner_draw = jnp.minimum(jax.random.randint(k_own_a, (SEL_DEV,), 0, TABLE_DEVS), jax.random.randint(k_own_b, (SEL_DEV,), 0, TABLE_DEVS))
    entry_draw = jnp.minimum(jax.random.randint(k_ent_a, (SEL_DEV,), 0, POOL_ROWS), jax.random.randint(k_ent_b, (SEL_DEV,), 0, POOL_ROWS))
    is_cover = sel_order < COVERED
    owner_idx = jnp.where(is_cover, sel_order // POOL_ROWS, owner_draw)
    entry_idx = jnp.where(is_cover, sel_order % POOL_ROWS, entry_draw)
    return dev_pool[owner_idx, entry_idx]


def draw_ids(ids_key):
    k_perm, k_common, k_shift, k_dev = jax.random.split(ids_key, 4)
    row_perm = jax.random.permutation(k_perm, BLOCK_ROWS)
    common = jax.random.randint(k_common, (TABLE_DEVS,), 0, BLOCK_ROWS)
    dev_shift = jax.random.randint(k_shift, (N_DEVS, TABLE_DEVS), 0, POOL_ROWS)
    offsets = (common[None, :, None] + dev_shift[:, :, None] + jnp.arange(POOL_ROWS)[None, None, :]) % BLOCK_ROWS
    row_pools = jnp.arange(TABLE_DEVS)[None, :, None] * BLOCK_ROWS + row_perm[offsets]
    picked = jax.vmap(one_device)(jax.random.split(k_dev, N_DEVS), row_pools)
    return picked.reshape(PART_TOKENS, N_HEADS, TOP_K).astype(jnp.int32)


def setup_inputs(seed: int = 0, part: int = 0) -> dict:
    part_key = jax.random.fold_in(jax.random.key(seed), part)
    k_tok, k_u, k_v, k_ids, k_gate, k_grad = jax.random.split(part_key, 6)
    tokens = jax.random.normal(k_tok, (PART_TOKENS, DIM_MODEL), jnp.float32).astype(jnp.bfloat16)
    table_u = (jax.random.normal(k_u, (EXPERTS, DIM_MODEL), jnp.float32) * DIM_MODEL ** -0.5).astype(jnp.bfloat16)
    table_v = jax.random.normal(k_v, (EXPERTS, DIM_MODEL), jnp.float32).astype(jnp.bfloat16)
    expert_ids = draw_ids(k_ids)
    gate_vals = jax.random.normal(k_gate, (PART_TOKENS, N_HEADS, TOP_K), jnp.float32) * SEL_TOK ** -0.5
    grad_out = jax.random.normal(k_grad, (PART_TOKENS, DIM_MODEL), jnp.float32).astype(jnp.bfloat16)
    return {'tokens': tokens, 'table_u': table_u, 'table_v': table_v, 'expert_ids': expert_ids, 'gate_vals': gate_vals, 'grad_out': grad_out}


def block_pass(tok_blk, grad_blk, ids_blk, gate_blk, table_u, table_v):
    id_grid = ids_blk.reshape(TOK_DEV, SEL_TOK)
    gate_grid = gate_blk.reshape(TOK_DEV, SEL_TOK)
    rows_u = jnp.take(table_u, id_grid, axis=0).astype(jnp.float32)
    rows_v = jnp.take(table_v, id_grid, axis=0).astype(jnp.float32)
    tok_wide = tok_blk.astype(jnp.float32)
    grad_wide = grad_blk.astype(jnp.float32)
    scores = jnp.einsum('td,tsd->ts', tok_wide, rows_u)
    act_val, act_slope = jax.jvp(jax.nn.gelu, (scores,), (jnp.ones_like(scores),))
    weight = (gate_grid * act_val).astype(jnp.bfloat16).astype(jnp.float32)
    out_y = jnp.einsum('ts,tsd->td', weight, rows_v).astype(jnp.bfloat16)
    back_dot = jnp.einsum('td,tsd->ts', grad_wide, rows_v)
    coef_bf = (gate_grid * act_slope * back_dot).astype(jnp.bfloat16).astype(jnp.float32)
    grad_x = jnp.einsum('ts,tsd->td', coef_bf, rows_u).astype(jnp.bfloat16)
    contrib_u = coef_bf[:, :, None] * tok_wide[:, None, :]
    contrib_v = weight[:, :, None] * grad_wide[:, None, :]
    return out_y, grad_x, id_grid.reshape(-1), contrib_u.reshape(-1, DIM_MODEL), contrib_v.reshape(-1, DIM_MODEL)


def reference(tokens, table_u, table_v, expert_ids, gate_vals, grad_out):
    n_blocks = tokens.shape[0] // TOK_DEV

    def scan_step(acc_pair, block_in):
        acc_u, acc_v = acc_pair
        out_y, grad_x, flat_ids, contrib_u, contrib_v = block_pass(block_in[0], block_in[1], block_in[2], block_in[3], table_u, table_v)
        return (acc_u.at[flat_ids].add(contrib_u), acc_v.at[flat_ids].add(contrib_v)), (out_y, grad_x)

    blocks = (tokens.reshape(n_blocks, TOK_DEV, DIM_MODEL), grad_out.reshape(n_blocks, TOK_DEV, DIM_MODEL), expert_ids.reshape(n_blocks, TOK_DEV, N_HEADS, TOP_K), gate_vals.reshape(n_blocks, TOK_DEV, N_HEADS, TOP_K))
    zero_acc = jnp.zeros((EXPERTS, DIM_MODEL), jnp.float32)
    (acc_u, acc_v), (out_rows, grad_rows) = lax.scan(scan_step, (zero_acc, zero_acc), blocks)
    return (out_rows.reshape(PART_TOKENS, DIM_MODEL), grad_rows.reshape(PART_TOKENS, DIM_MODEL), acc_u.astype(jnp.bfloat16), acc_v.astype(jnp.bfloat16))
```

```python
import functools

import jax
import jax.numpy as jnp
from jax import lax
from jax.experimental import pallas as pl
from jax.experimental.pallas import tpu as pltpu
from jax.sharding import PartitionSpec as P


LANES = 128
SUB = 128
WIDE = 512
Q_COMBINE = 6
Q_GRAD = 8
VMEM_BYTES = 64 * 1024 * 1024 - 128 * 1024
NT = (((1,), (1,)), ((), ()))
NN = (((1,), (0,)), ((), ()))


def lane_take(values, idx):
    return jnp.take_along_axis(values, idx, axis=1, mode='promise_in_bounds')


def lower_bound(keys, target):
    pos = jnp.zeros_like(target)
    step = LANES // 2
    while step >= 1:
        probe = lane_take(keys, pos + (step - 1))
        pos = jnp.where(probe < target, pos + step, pos)
        step //= 2
    return pos + (lane_take(keys, pos) < target).astype(jnp.int32)


def lane_iota(rows):
    return lax.broadcasted_iota(jnp.int32, (rows, LANES), 1)


def prep_kernel(ids_ref, enc_ref, tab_ref):
    lane = lane_iota(8)

    def group(g, carry):
        dup_max, len_max = carry
        rows = pl.ds(pl.multiple_of(g * 8, 8), 8)
        keys = ids_ref[rows, :]
        rank = lane - lower_bound(keys, keys)
        enc_ref[rows, :] = (keys * LANES + rank).astype(jnp.float32)
        dup_sum = (rank > 0).astype(jnp.int32)
        step = 1
        while step < LANES:
            dup_sum = dup_sum + jnp.where(lane >= step, pltpu.roll(dup_sum, step, 1), 0)
            step *= 2
        per = WIDE // SUB
        marks = [lower_bound(keys, lane * WIDE + part * SUB) for part in range(per + 1)]
        for part in range(per):
            len_max = jnp.maximum(len_max, marks[part + 1] - marks[part])
        ends = [jnp.where(m > 0, lane_take(dup_sum, jnp.maximum(m - 1, 0)), 0) for m in (marks[0], marks[per])]
        return jnp.maximum(dup_max, ends[1] - ends[0]), len_max

    zero = jnp.zeros((8, LANES), jnp.int32)
    dup_max, len_max = lax.fori_loop(0, ids_ref.shape[0] // 8, group, (zero, zero))
    dup_row = jnp.max(dup_max, axis=0, keepdims=True) + 1
    len_row = jnp.max(len_max, axis=0, keepdims=True)
    first = lax.broadcasted_iota(jnp.int32, (8, LANES), 0) == 0
    tab_ref[...] = jnp.where(first, dup_row, len_row).astype(jnp.float32)


def prepare(ids_sorted):
    n_tok, sel = ids_sorted.shape
    return pl.pallas_call(
        prep_kernel,
        out_shape=(jax.ShapeDtypeStruct((n_tok, sel), jnp.float32), jax.ShapeDtypeStruct((8, LANES), jnp.float32)),
        name='prep',
    )(ids_sorted)


def score_kernel(block_rows, x_ref, dy_ref, u_ref, v_ref, enc_ref, gate_ref, wc_ref, a_acc, b_acc, sa0, sb0, sa1, sb1):
    chunk = pl.program_id(0)
    n_tok = x_ref.shape[0]
    tile = sa0.shape[0]
    n_tile = n_tok // tile
    per = WIDE // SUB
    bufs = ((sa0, sb0), (sa1, sb1))

    @pl.when(chunk == 0)
    def _():
        a_acc[...] = jnp.zeros_like(a_acc)
        b_acc[...] = jnp.zeros_like(b_acc)

    def dots(t):
        sa, sb = bufs[t % 2]
        rows = slice(t * tile, (t + 1) * tile)
        sa[...] = lax.dot_general(x_ref[rows, :], u_ref[...], NT, preferred_element_type=jnp.float32)
        sb[...] = lax.dot_general(dy_ref[rows, :], v_ref[...], NT, preferred_element_type=jnp.float32)

    def pick(t):
        sa, sb = bufs[t % 2]
        for g in range(tile // 8):
            rows = slice(t * tile + g * 8, t * tile + g * 8 + 8)
            loc = slice(g * 8, g * 8 + 8)
            row_id = enc_ref[rows, :] >> 7
            lo = row_id & (LANES - 1)
            hi = (row_id >> 7) - chunk * per
            a_val, b_val = a_acc[rows, :], b_acc[rows, :]
            for h in range(per):
                cols = slice(h * LANES, (h + 1) * LANES)
                hit = hi == h
                a_val = jnp.where(hit, lane_take(sa[loc, cols], lo), a_val)
                b_val = jnp.where(hit, lane_take(sb[loc, cols], lo), b_val)
            a_acc[rows, :] = a_val
            b_acc[rows, :] = b_val

    dots(0)
    for t in range(n_tile):
        if t + 1 < n_tile:
            dots(t + 1)
        pick(t)

    @pl.when(chunk == pl.num_programs(0) - 1)
    def _():
        step = min(64, n_tok)

        def finish(i, _):
            rows = pl.ds(pl.multiple_of(i * step, step), step)
            a_val, gate = a_acc[rows, :], gate_ref[rows, :]
            act, slope = jax.jvp(jax.nn.gelu, (a_val,), (jnp.ones_like(a_val),))
            row_id = enc_ref[rows, :] >> 7
            mine = (row_id >= 0) & (row_id < block_rows)
            weight = jnp.where(mine, gate * act, 0.0)
            coef = jnp.where(mine, gate * slope * b_acc[rows, :], 0.0)
            wc_ref[rows, :LANES] = weight.astype(jnp.bfloat16)
            wc_ref[rows, LANES:] = coef.astype(jnp.bfloat16)
            return 0

        lax.fori_loop(0, n_tok // step, finish, 0)


def scores(tok_pair, table_u, table_v, enc, gate):
    n_tok, pair_width = tok_pair.shape
    width = pair_width // 2
    block_rows = table_u.shape[0]
    tile = min(512, n_tok)
    whole = lambda shape: pl.BlockSpec(shape, lambda c: (0, 0))
    return pl.pallas_call(
        functools.partial(score_kernel, block_rows),
        grid=(block_rows // WIDE,),
        in_specs=[
            pl.BlockSpec((n_tok, width), lambda c: (0, 0)),
            pl.BlockSpec((n_tok, width), lambda c: (0, 1)),
            pl.BlockSpec((WIDE, width), lambda c: (c, 0)),
            pl.BlockSpec((WIDE, width), lambda c: (c, 0)),
            whole((n_tok, LANES)),
            whole((n_tok, LANES)),
        ],
        out_specs=whole((n_tok, 2 * LANES)),
        out_shape=jax.ShapeDtypeStruct((n_tok, 2 * LANES), jnp.bfloat16),
        scratch_shapes=[pltpu.VMEM((n_tok, LANES), jnp.float32)] * 2 + [pltpu.VMEM((tile, WIDE), jnp.float32)] * 4,
        compiler_params=pltpu.CompilerParams(vmem_limit_bytes=VMEM_BYTES),
        cost_estimate=pl.CostEstimate(flops=4 * n_tok * block_rows * width, bytes_accessed=8 * block_rows * width, transcendentals=0),
        name='scores',
    )(tok_pair, tok_pair, table_u, table_v, enc, gate)


def expand_lists(enc_ref, wc_ref, tok0, n_tok, n_sub, n_lane_tile, q_base, tmps, outs, out_row):
    q_per = LANES // n_sub
    lane = lane_iota(8)
    chunk_of = lane & (n_sub - 1)
    q_of = lane // n_sub
    target = chunk_of * (SUB * LANES)
    for g in range(n_tok // 8):
        rows = pl.ds(pl.multiple_of(tok0 + g * 8, 8), 8)
        loc = slice(g * 8, g * 8 + 8)
        enc = enc_ref[rows, :]
        weight = wc_ref[rows, :LANES].astype(jnp.float32)
        coef = wc_ref[rows, LANES:].astype(jnp.float32)
        start = lower_bound(enc, target) + q_of + q_base
        for t in range(n_lane_tile):
            idx = start + t * q_per
            safe = jnp.minimum(idx, LANES - 1)
            got = lane_take(enc, safe)
            valid = (idx < LANES) & ((got >> 14) == chunk_of)
            place = ((got >> 7) & (SUB - 1)) + SUB * (got & (LANES - 1))
            tmps[0][t, loc, :] = jnp.where(valid, place, -1).astype(jnp.float32)
            tmps[1][t, loc, :] = lane_take(weight, safe)
            tmps[2][t, loc, :] = lane_take(coef, safe)
    for t in range(n_lane_tile):
        for tmp, out in zip(tmps, outs):
            out[pl.ds(pl.multiple_of(out_row + t * LANES, LANES), LANES), :] = tmp[t].T


def densify(lists, base, chunk0, n_sub, n_q, layer, outs):
    n_tok = lists[0].shape[1]
    row16 = lax.broadcasted_iota(jnp.int32, (16, n_tok), 0).astype(jnp.float32)
    for part in range(WIDE // SUB):
        place, weight, coef = [], [], []
        for q in range(n_q):
            row = pl.ds(base + q * n_sub + chunk0 + part, 1)
            shift = jnp.asarray(layer * SUB, jnp.float32)
            place.append(jnp.broadcast_to(lists[0][row, :] - shift, (16, n_tok)).astype(jnp.bfloat16))
            weight.append(jnp.broadcast_to(lists[1][row, :], (16, n_tok)).astype(jnp.bfloat16))
            coef.append(jnp.broadcast_to(lists[2][row, :], (16, n_tok)).astype(jnp.bfloat16))
        for b in range(SUB // 16):
            mine = (row16 + 16 * b).astype(jnp.bfloat16)
            w_val = jnp.zeros((16, n_tok), jnp.bfloat16)
            c_val = jnp.zeros((16, n_tok), jnp.bfloat16)
            for q in range(n_q):
                hit = place[q] == mine
                w_val = jnp.where(hit, weight[q], w_val)
                c_val = jnp.where(hit, coef[q], c_val)
            rows = slice(part * SUB + 16 * b, part * SUB + 16 * b + 16)
            outs[0][rows, :] = w_val
            outs[1][rows, :] = c_val


def combine_kernel(n_tok, n_sub, tab_ref, u_ref, v_ref, enc_ref, wc_ref, out_ref,
                   le, lw, lc, se, sw, sc, te, tw, tc, acc_y, acc_dx, vt, ut, w0, c0, w1, c1, w2, c2, sem):
    chunk = pl.program_id(0)
    n_chunk = pl.num_programs(0)
    n_tile = acc_y.shape[0]
    n_lane_tile = te.shape[0]
    n_q = n_lane_tile * (LANES // n_sub)
    n_row = n_q * n_sub
    lists, spare, tmps = (le, lw, lc), (se, sw, sc), (te, tw, tc)
    per = WIDE // SUB
    chunk0 = chunk * per

    @pl.when(chunk == 0)
    def _():
        def start(i, _):
            acc_y[i] = jnp.zeros(acc_y.shape[1:], jnp.float32)
            acc_dx[i] = jnp.zeros(acc_dx.shape[1:], jnp.float32)
            expand_lists(enc_ref, wc_ref, i * n_tok, n_tok, n_sub, n_lane_tile, 0, tmps, lists, i * n_row)
            return 0

        lax.fori_loop(0, n_tile, start, 0)

    vt[...] = v_ref[...].T
    ut[...] = u_ref[...].T

    def dense(i, bufs):
        densify(lists, i * n_row, chunk0, n_sub, n_q, 0, bufs)

    def add(i, bufs):
        acc_y[i] += lax.dot_general(vt[...], bufs[0][...], NN, preferred_element_type=jnp.float32)
        acc_dx[i] += lax.dot_general(ut[...], bufs[1][...], NN, preferred_element_type=jnp.float32)

    def rest(i):
        n_layer = tab_ref[0, i * n_chunk + chunk]
        n_long = tab_ref[1, i * n_chunk + chunk]

        def layer_step(r, _):
            densify(lists, i * n_row, chunk0, n_sub, n_q, r, (w2, c2))
            add(i, (w2, c2))
            return 0

        lax.fori_loop(1, n_layer, layer_step, 0)

        def long_step(qb, _):
            expand_lists(enc_ref, wc_ref, i * n_tok, n_tok, n_sub, n_lane_tile, qb * n_q, tmps, spare, 0)

            def spare_step(r, _):
                densify(spare, 0, chunk0, n_sub, n_q, r, (w2, c2))
                add(i, (w2, c2))
                return 0

            lax.fori_loop(0, n_layer, spare_step, 0)
            return 0

        lax.fori_loop(1, (n_long + n_q - 1) // n_q, long_step, 0)

    dense(0, (w0, c0))

    def pair(p, _):
        i = 2 * p
        dense(i + 1, (w1, c1))
        add(i, (w0, c0))
        rest(i)
        dense(jnp.minimum(i + 2, n_tile - 1), (w0, c0))
        add(i + 1, (w1, c1))
        rest(i + 1)
        return 0

    lax.fori_loop(0, n_tile // 2, pair, 0)

    @pl.when(chunk == n_chunk - 1)
    def _():
        for i in range(n_tile):
            pltpu.make_async_copy(acc_y.at[i], out_ref.at[i, 0], sem.at[0]).start()
            pltpu.make_async_copy(acc_dx.at[i], out_ref.at[i, 1], sem.at[0]).start()
        for i in range(n_tile):
            pltpu.make_async_copy(acc_y.at[i], out_ref.at[i, 0], sem.at[0]).wait()
            pltpu.make_async_copy(acc_dx.at[i], out_ref.at[i, 1], sem.at[0]).wait()


def combine(n_tile, tab, table_u, table_v, enc, wc):
    block_rows, width = table_u.shape
    n_all = enc.shape[0]
    n_tok = n_all // n_tile
    n_sub = block_rows // SUB
    q_per = LANES // n_sub
    n_lane_tile = -(-Q_COMBINE // q_per)
    n_row = n_lane_tile * LANES
    f32, bf16 = jnp.float32, jnp.bfloat16
    return pl.pallas_call(
        functools.partial(combine_kernel, n_tok, n_sub),
        grid_spec=pltpu.PrefetchScalarGridSpec(
            num_scalar_prefetch=1,
            grid=(block_rows // WIDE,),
            in_specs=[
                pl.BlockSpec((WIDE, width), lambda c, t: (c, 0)),
                pl.BlockSpec((WIDE, width), lambda c, t: (c, 0)),
                pl.BlockSpec((n_all, LANES), lambda c, t: (0, 0)),
                pl.BlockSpec((n_all, 2 * LANES), lambda c, t: (0, 0)),
            ],
            out_specs=pl.BlockSpec(memory_space=pl.ANY),
            scratch_shapes=[pltpu.VMEM((n_tile * n_row, n_tok), f32)] * 3
            + [pltpu.VMEM((n_row, n_tok), f32)] * 3
            + [pltpu.VMEM((n_lane_tile, n_tok, LANES), f32)] * 3
            + [pltpu.VMEM((n_tile, width, n_tok), f32)] * 2
            + [pltpu.VMEM((width, WIDE), bf16)] * 2
            + [pltpu.VMEM((WIDE, n_tok), bf16)] * 6
            + [pltpu.SemaphoreType.DMA((1,))],
        ),
        out_shape=jax.ShapeDtypeStruct((n_tile, 2, width, n_tok), f32),
        compiler_params=pltpu.CompilerParams(vmem_limit_bytes=VMEM_BYTES),
        cost_estimate=pl.CostEstimate(flops=4 * n_all * block_rows * width, bytes_accessed=12 * n_all * width, transcendentals=0),
        name='combine',
    )(tab, table_u, table_v, enc, wc)


def grad_kernel(n_sub, tab_ref, x_ref, dy_ref, enc_ref, wc_ref, du_ref, dv_ref,
                le, lw, lc, te, tw, tc, acc_u, acc_v, w0, c0, w1, c1, w2, c2):
    step = pl.program_id(0)
    n_tok = x_ref.shape[0]
    n_lane_tile = te.shape[0]
    n_q = n_lane_tile * (LANES // n_sub)
    lists, tmps = (le, lw, lc), (te, tw, tc)
    per = WIDE // SUB
    n_chunk = acc_u.shape[0] // WIDE
    bufs = ((w0, c0), (w1, c1))

    @pl.when(step == 0)
    def _():
        acc_u[...] = jnp.zeros_like(acc_u)
        acc_v[...] = jnp.zeros_like(acc_v)

    def add(k, pair):
        rows = slice(k * WIDE, (k + 1) * WIDE)
        acc_v[rows, :] += lax.dot_general(pair[0][...], dy_ref[...], NN, preferred_element_type=jnp.float32)
        acc_u[rows, :] += lax.dot_general(pair[1][...], x_ref[...], NN, preferred_element_type=jnp.float32)

    n_long = tab_ref[1, step * n_chunk]
    for k in range(1, n_chunk):
        n_long = jnp.maximum(n_long, tab_ref[1, step * n_chunk + k])

    def list_block(qb, _):
        expand_lists(enc_ref, wc_ref, 0, n_tok, n_sub, n_lane_tile, qb * n_q, tmps, lists, 0)
        densify(lists, 0, 0, n_sub, n_q, 0, bufs[0])
        for k in range(n_chunk):
            if k + 1 < n_chunk:
                densify(lists, 0, (k + 1) * per, n_sub, n_q, 0, bufs[(k + 1) % 2])
            add(k, bufs[k % 2])
        for k in range(n_chunk):
            def layer_step(r, _):
                densify(lists, 0, k * per, n_sub, n_q, r, (w2, c2))
                add(k, (w2, c2))
                return 0

            lax.fori_loop(1, tab_ref[0, step * n_chunk + k], layer_step, 0)
        return 0

    lax.fori_loop(0, (n_long + n_q - 1) // n_q, list_block, 0)

    @pl.when(step == pl.num_programs(0) - 1)
    def _():
        du_ref[...] = acc_u[...].astype(jnp.bfloat16)
        dv_ref[...] = acc_v[...].astype(jnp.bfloat16)


def table_grads(own_rows, tab, tok_pair, enc, wc):
    n_all, pair_width = tok_pair.shape
    width = pair_width // 2
    tile = min(512, n_all)
    n_sub = own_rows // SUB
    q_per = LANES // n_sub
    n_lane_tile = -(-Q_GRAD // q_per)
    n_row = n_lane_tile * LANES
    f32, bf16 = jnp.float32, jnp.bfloat16
    out = jax.ShapeDtypeStruct((own_rows, width), bf16)
    return pl.pallas_call(
        functools.partial(grad_kernel, n_sub),
        grid_spec=pltpu.PrefetchScalarGridSpec(
            num_scalar_prefetch=1,
            grid=(n_all // tile,),
            in_specs=[
                pl.BlockSpec((tile, width), lambda s, t: (s, 0)),
                pl.BlockSpec((tile, width), lambda s, t: (s, 1)),
                pl.BlockSpec((tile, LANES), lambda s, t: (s, 0)),
                pl.BlockSpec((tile, 2 * LANES), lambda s, t: (s, 0)),
            ],
            out_specs=[pl.BlockSpec((own_rows, width), lambda s, t: (0, 0))] * 2,
            scratch_shapes=[pltpu.VMEM((n_row, tile), f32)] * 3
            + [pltpu.VMEM((n_lane_tile, tile, LANES), f32)] * 3
            + [pltpu.VMEM((own_rows, width), f32)] * 2
            + [pltpu.VMEM((WIDE, tile), bf16)] * 6,
        ),
        out_shape=(out, out),
        compiler_params=pltpu.CompilerParams(vmem_limit_bytes=VMEM_BYTES),
        cost_estimate=pl.CostEstimate(flops=4 * n_all * own_rows * width, bytes_accessed=4 * n_all * width, transcendentals=0),
        name='table_grads',
    )(tab, tok_pair, tok_pair, enc, wc)


def solution(mesh):
    owners = mesh.shape['table']
    copies = mesh.shape['data']
    tok_spec = P(('rep', 'data', 'table'), None)
    sel_spec = P(('rep', 'data', 'table'), None, None)
    row_spec = P(('rep', 'table'), None)
    grad_spec = P(('rep', 'table', 'data'), None)

    def device_fn(tokens, table_u, table_v, expert_ids, gate_vals, grad_out):
        n_tok, _ = tokens.shape
        sel = expert_ids.shape[1] * expert_ids.shape[2]
        block_rows = table_u.shape[0]
        own_rows = block_rows // copies
        my_block = lax.axis_index('table')
        my_copy = lax.axis_index('data')

        ids_sorted, gates = lax.sort((expert_ids.reshape(n_tok, sel), gate_vals.reshape(n_tok, sel)), dimension=1, num_keys=1)
        enc, tab = prepare(ids_sorted)
        lists = jnp.concatenate([enc, tab], axis=0)
        lists_gates = jnp.concatenate([lists, jnp.concatenate([gates, jnp.zeros((tab.shape[0], sel), jnp.float32)], axis=0)], axis=1)
        pair = jnp.concatenate([tokens, grad_out], axis=1)

        row_q = lax.all_gather(lists_gates, 'table', axis=0, tiled=False)
        row_pair = lax.all_gather(pair, 'table', axis=0, tiled=True)
        row_enc = row_q[:, :n_tok, :sel].reshape(owners * n_tok, sel).astype(jnp.int32) - my_block * (block_rows * LANES)
        row_gate = row_q[:, :n_tok, sel:].reshape(owners * n_tok, sel)
        n_chunk = block_rows // WIDE
        row_tab = lax.dynamic_slice_in_dim(row_q[:, n_tok:n_tok + 2, :sel], my_block * n_chunk, n_chunk, 2)
        row_tab = row_tab.transpose(1, 0, 2).reshape(2, owners * n_chunk).astype(jnp.int32)

        late_pair, late_lists, row_pair = lax.optimization_barrier((pair, lists, row_pair))
        all_lists = lax.all_gather(late_lists, ('data', 'table'), axis=0, tiled=False)
        all_pair = lax.all_gather(late_pair, ('data', 'table'), axis=0, tiled=True)

        wc = scores(row_pair, table_u, table_v, row_enc, row_gate)
        all_wc = lax.all_gather(wc, 'data', axis=0, tiled=True)
        part = combine(owners, row_tab, table_u, table_v, row_enc, wc)
        own = lax.psum_scatter(part, 'table', scatter_dimension=0, tiled=True)[0]

        first_row = my_block * block_rows + my_copy * own_rows
        all_enc = all_lists[:, :n_tok, :].reshape(-1, sel).astype(jnp.int32) - first_row * LANES
        n_own = own_rows // WIDE
        all_tab = lax.dynamic_slice_in_dim(all_lists[:, n_tok:n_tok + 2, :], first_row // WIDE, n_own, 2)
        tile = min(512, owners * copies * n_tok)
        all_tab = all_tab.reshape(-1, tile // n_tok, 2, n_own).max(axis=1).transpose(1, 0, 2).reshape(2, -1).astype(jnp.int32)
        grad_u, grad_v = table_grads(own_rows, all_tab, all_pair, all_enc, all_wc)
        return own[0].T.astype(jnp.bfloat16), own[1].T.astype(jnp.bfloat16), grad_u, grad_v

    return jax.shard_map(device_fn, mesh=mesh, in_specs=(tok_spec, row_spec, row_spec, sel_spec, sel_spec, tok_spec), out_specs=(tok_spec, tok_spec, grad_spec, grad_spec), check_vma=False)
```

```python
import functools

import jax
import jax.numpy as jnp
from jax import lax
from jax.experimental import pallas as pl
from jax.experimental.pallas import tpu as pltpu
from jax.sharding import PartitionSpec as P


LANES = 128
SUB = 128
WIDE = 512
MERGED = 4
REP_ROWS = 4
REP_TOKEN = 16
WINDOW = 128
BLOCK = 256
BIG = 2 ** 31 - 1


def log2(n):
    assert n & (n - 1) == 0
    return n.bit_length() - 1


VMEM_BYTES = 64 * 1024 * 1024 - 128 * 1024
NT = (((1,), (1,)), ((), ()))
NN = (((1,), (0,)), ((), ()))


def lane_take(values, idx):
    return jnp.take_along_axis(values, idx, axis=1, mode='promise_in_bounds')


def lower_bound(keys, target):
    pos = jnp.zeros_like(target)
    step = LANES // 2
    while step >= 1:
        probe = lane_take(keys, pos + (step - 1))
        pos = jnp.where(probe < target, pos + step, pos)
        step //= 2
    return pos + (lane_take(keys, pos) < target).astype(jnp.int32)


def find_starts(enc_ref, out_ref, groups, n_sub):
    target = (lane_iota(8) & (n_sub - 1)) * (SUB * LANES)
    for g in groups:
        rows = pl.ds(pl.multiple_of(g * 8, 8), 8)
        out_ref[rows, :] = lower_bound(enc_ref[rows, :], target)


def lane_iota(rows):
    return lax.broadcasted_iota(jnp.int32, (rows, LANES), 1)


def prep_kernel(ids_ref, enc_ref, tab_ref, key_ref):
    lane = lane_iota(8)
    row = lax.broadcasted_iota(jnp.int32, (8, LANES), 0)
    n_place = ids_ref.shape[0] * LANES
    together = min(8, ids_ref.shape[0] // 8)

    def group(g, carry):
        most_rank, most_len, total, most_rest = carry
        rows = pl.ds(pl.multiple_of(g * 8, 8), 8)
        keys = ids_ref[rows, :]
        rank = lane - lower_bound(keys, keys)
        nth = lane - lower_bound(keys, keys & -SUB)
        enc_ref[rows, :] = (keys * LANES + rank).astype(jnp.float32)
        rest = ((rank > 0) | (nth >= MERGED)).astype(jnp.int32)
        count = rest
        step = 1
        while step < LANES:
            count = count + jnp.where(lane >= step, pltpu.roll(count, step, 1), 0)
            step *= 2
        source = lower_bound(count, lane + 1)
        safe = jnp.minimum(source, LANES - 1)
        place = (g * 8 + row) * LANES + safe
        key_ref[rows, :] = jnp.where(source < LANES, lane_take(keys, safe) * n_place + place, BIG)
        return jnp.maximum(most_rank, rank), jnp.maximum(most_len, nth), total + rest, jnp.maximum(most_rest, count)

    def groups(i, carry):
        for j in range(together):
            carry = group(i * together + j, carry)
        return carry

    zero = jnp.zeros((8, LANES), jnp.int32)
    found = lax.fori_loop(0, ids_ref.shape[0] // (8 * together), groups, (zero, zero, zero, zero))
    out = jnp.zeros((8, LANES), jnp.float32)
    for i, (value, op) in enumerate(zip(found, (jnp.max, jnp.max, jnp.sum, jnp.max))):
        one = op(op(value.astype(jnp.float32), axis=0, keepdims=True), axis=1, keepdims=True)
        out = jnp.where(row == i, one, out)
    tab_ref[...] = out


def prepare(ids_sorted):
    n_tok, sel = ids_sorted.shape
    return pl.pallas_call(
        prep_kernel,
        out_shape=(jax.ShapeDtypeStruct((n_tok, sel), jnp.float32), jax.ShapeDtypeStruct((8, LANES), jnp.float32),
                   jax.ShapeDtypeStruct((n_tok, sel), jnp.int32)),
        name='prep',
    )(ids_sorted)


def score_kernel(block_rows, n_chunk, x_ref, dy_ref, u_ref, v_ref, enc_ref, gate_ref, wc_ref, start_ref, a_acc, b_acc, sa0, sb0, sa1, sb1):
    chunk = pl.program_id(0)
    n_tok = x_ref.shape[0]
    tile = sa0.shape[0]
    n_tile = n_tok // tile
    per = WIDE // SUB
    bufs = ((sa0, sb0), (sa1, sb1))

    @pl.when(chunk == 0)
    def _():
        a_acc[...] = jnp.zeros_like(a_acc)
        b_acc[...] = jnp.zeros_like(b_acc)

    def dots(t):
        sa, sb = bufs[t % 2]
        rows = slice(t * tile, (t + 1) * tile)
        sa[...] = lax.dot_general(x_ref[rows, :], u_ref[...], NT, preferred_element_type=jnp.float32)
        sb[...] = lax.dot_general(dy_ref[rows, :], v_ref[...], NT, preferred_element_type=jnp.float32)

    def pick(t):
        sa, sb = bufs[t % 2]
        for g in range(tile // 8):
            rows = slice(t * tile + g * 8, t * tile + g * 8 + 8)
            loc = slice(g * 8, g * 8 + 8)
            row_id = enc_ref[rows, :] >> 7
            lo = row_id & (LANES - 1)
            hi = (row_id >> 7) - chunk * per
            a_val, b_val = a_acc[rows, :], b_acc[rows, :]
            for h in range(per):
                cols = slice(h * LANES, (h + 1) * LANES)
                hit = hi == h
                a_val = jnp.where(hit, lane_take(sa[loc, cols], lo), a_val)
                b_val = jnp.where(hit, lane_take(sb[loc, cols], lo), b_val)
            a_acc[rows, :] = a_val
            b_acc[rows, :] = b_val

    share = n_tok // (8 * n_chunk * n_tile)
    dots(0)
    for t in range(n_tile):
        if t + 1 < n_tile:
            dots(t + 1)
        pick(t)
        find_starts(enc_ref, start_ref, [(chunk * n_tile + t) * share + j for j in range(share)], block_rows // SUB)

    @pl.when(chunk == pl.num_programs(0) - 1)
    def _():
        step = min(64, n_tok)

        def finish(i, _):
            rows = pl.ds(pl.multiple_of(i * step, step), step)
            a_val, gate = a_acc[rows, :], gate_ref[rows, :]
            act, slope = jax.jvp(jax.nn.gelu, (a_val,), (jnp.ones_like(a_val),))
            row_id = enc_ref[rows, :] >> 7
            mine = (row_id >= 0) & (row_id < block_rows)
            weight = jnp.where(mine, gate * act, 0.0)
            coef = jnp.where(mine, gate * slope * b_acc[rows, :], 0.0)
            wc_ref[rows, :LANES] = weight.astype(jnp.bfloat16)
            wc_ref[rows, LANES:] = coef.astype(jnp.bfloat16)
            return 0

        lax.fori_loop(0, n_tok // step, finish, 0)


def scores(tok_pair, table_u, table_v, enc, gate):
    n_tok, pair_width = tok_pair.shape
    width = pair_width // 2
    block_rows = table_u.shape[0]
    tile = min(512, n_tok)
    whole = lambda shape: pl.BlockSpec(shape, lambda c: (0, 0))
    return pl.pallas_call(
        functools.partial(score_kernel, block_rows, block_rows // WIDE),
        grid=(block_rows // WIDE,),
        in_specs=[
            pl.BlockSpec((n_tok, width), lambda c: (0, 0)),
            pl.BlockSpec((n_tok, width), lambda c: (0, 1)),
            pl.BlockSpec((WIDE, width), lambda c: (c, 0)),
            pl.BlockSpec((WIDE, width), lambda c: (c, 0)),
            whole((n_tok, LANES)),
            whole((n_tok, LANES)),
        ],
        out_specs=(whole((n_tok, 2 * LANES)), whole((n_tok, LANES))),
        out_shape=(jax.ShapeDtypeStruct((n_tok, 2 * LANES), jnp.bfloat16), jax.ShapeDtypeStruct((n_tok, LANES), jnp.int32)),
        scratch_shapes=[pltpu.VMEM((n_tok, LANES), jnp.float32)] * 2 + [pltpu.VMEM((tile, WIDE), jnp.float32)] * 4,
        compiler_params=pltpu.CompilerParams(vmem_limit_bytes=VMEM_BYTES),
        cost_estimate=pl.CostEstimate(flops=4 * n_tok * block_rows * width, bytes_accessed=8 * block_rows * width, transcendentals=0),
        name='scores',
    )(tok_pair, tok_pair, table_u, table_v, enc, gate)


def expand_groups(enc_ref, wc_ref, start_ref, tok0, groups, n_sub, q_base, tmps):
    q_per = LANES // n_sub
    lane = lane_iota(8)
    chunk_of = lane & (n_sub - 1)
    q_of = lane >> log2(n_sub)
    for g in groups:
        rows = pl.ds(pl.multiple_of(tok0 + g * 8, 8), 8)
        loc = pl.ds(pl.multiple_of(g * 8, 8), 8) if not isinstance(g, int) else slice(g * 8, g * 8 + 8)
        enc = enc_ref[rows, :]
        weight = wc_ref[rows, :LANES].astype(jnp.float32)
        coef = wc_ref[rows, LANES:].astype(jnp.float32)
        start = start_ref[rows, :] + q_of + q_base
        for t in range(tmps[0].shape[0]):
            idx = start + t * q_per
            safe = jnp.minimum(idx, LANES - 1)
            got = lane_take(enc, safe)
            valid = (idx < LANES) & ((got >> 14) == chunk_of)
            place = ((got >> 7) & (SUB - 1)) + SUB * (got & (LANES - 1))
            tmps[0][t, loc, :] = jnp.where(valid, place, -1).astype(jnp.float32)
            tmps[1][t, loc, :] = lane_take(weight, safe)
            tmps[2][t, loc, :] = lane_take(coef, safe)


def turn_lists(tmps, outs, out_row):
    for t in range(tmps[0].shape[0]):
        rows = slice(out_row + t * LANES, out_row + (t + 1) * LANES) if isinstance(out_row, int) else pl.ds(pl.multiple_of(out_row + t * LANES, LANES), LANES)
        for tmp, out in zip(tmps, outs):
            out[rows, :] = tmp[t].T


def expand_slowly(enc_ref, wc_ref, start_ref, tok0, n_tok, n_sub, q_base, tmps, outs):
    def some(g, _):
        expand_groups(enc_ref, wc_ref, start_ref, tok0, [g], n_sub, q_base, tmps)
        return 0

    lax.fori_loop(0, n_tok // 8, some, 0)
    turn_lists(tmps, outs, 0)


def fill_tile(entries, n_col, part, outs):
    spread = [[jnp.broadcast_to(v, (16, n_col)).astype(jnp.bfloat16) for v in entry] for entry in entries]
    row16 = lax.broadcasted_iota(jnp.int32, (16, n_col), 0).astype(jnp.float32)
    for b in range(SUB // 16):
        mine = (row16 + 16 * b).astype(jnp.bfloat16)
        w_val = jnp.zeros((16, n_col), jnp.bfloat16)
        c_val = jnp.zeros((16, n_col), jnp.bfloat16)
        for place, weight, coef in spread:
            hit = place == mine
            w_val = jnp.where(hit, weight, w_val)
            c_val = jnp.where(hit, coef, c_val)
        rows = slice(part * SUB + 16 * b, part * SUB + 16 * b + 16)
        outs[0][rows, :n_col] = w_val
        outs[1][rows, :n_col] = c_val


def densify(lists, base, chunk0, n_sub, layer, outs):
    shift = jnp.asarray(layer * SUB, jnp.float32)
    for part in range(WIDE // SUB):
        entries = []
        for q in range(MERGED):
            row = pl.ds(base + q * n_sub + chunk0 + part, 1)
            entries.append((lists[0][row, :] - shift, lists[1][row, :], lists[2][row, :]))
        fill_tile(entries, lists[0].shape[1], part, outs)


def one_hot_rows(pick, n_col, out):
    lane = lane_iota(pick.shape[0])
    for part in range(n_col // LANES):
        hit = pick == lane + part * LANES
        out[:, part * LANES:(part + 1) * LANES] = jnp.where(hit, 1.0, 0.0).astype(jnp.bfloat16)


def combine_kernel(n_tok, n_sub, n_chunks, own_sub, tab_ref, off_ref, u_ref, v_ref, enc_ref, wc_ref, start_ref, slot_ref, all_enc_ref, out_ref, all_start_ref,
                   le, lw, lc, te, tw, tc, se, sw, sc, re, rw, rc, acc_y, acc_dx, vt, ut, w0, c0, w1, c1, w2, c2,
                   u_rep, v_rep, hot, wx, cx, sem):
    chunk = pl.program_id(0)
    n_chunk = pl.num_programs(0)
    n_tile = acc_y.shape[0]
    n_row = te.shape[0] * LANES
    lists, tmps, spare, spare_tmps = (le, lw, lc), (te, tw, tc), (se, sw, sc), (re, rw, rc)
    per = WIDE // SUB
    chunk0 = chunk * per

    @pl.when(chunk == 0)
    def _():
        def start(i, _):
            acc_y[i] = jnp.zeros(acc_y.shape[1:], jnp.float32)
            acc_dx[i] = jnp.zeros(acc_dx.shape[1:], jnp.float32)
            expand_groups(enc_ref, wc_ref, start_ref, i * n_tok, range(n_tok // 8), n_sub, 0, tmps)
            turn_lists(tmps, lists, i * n_row)
            return 0

        lax.fori_loop(0, n_tile, start, 0)
        u_rep[...] = jnp.zeros_like(u_rep)
        v_rep[...] = jnp.zeros_like(v_rep)

    vt[...] = v_ref[...].T
    ut[...] = u_ref[...].T

    def dense(i, bufs):
        last = i >= n_tile
        tile = jnp.where(last, 0, i)
        densify(lists, tile * n_row, jnp.where(last, jnp.minimum(chunk + 1, n_chunk - 1), chunk) * per, n_sub, 0, bufs)

    def add(i, bufs):
        acc_y[i] += lax.dot_general(vt[...], bufs[0][...], NN, preferred_element_type=jnp.float32)
        acc_dx[i] += lax.dot_general(ut[...], bufs[1][...], NN, preferred_element_type=jnp.float32)

    def rest(i, _):
        n_layer, n_long = tab_ref[0, i], tab_ref[1, i]

        def list_block(qb, _):
            expand_slowly(enc_ref, wc_ref, start_ref, i * n_tok, n_tok, n_sub, qb * MERGED, spare_tmps, spare)

            def layer_step(r, _):
                densify(spare, 0, chunk0, n_sub, r, (w2, c2))
                add(i, (w2, c2))
                return 0

            lax.fori_loop(jnp.where(qb == 0, 1, 0), n_layer, layer_step, 0)
            return 0

        @pl.when((n_layer > 1) | (n_long > MERGED))
        def _():
            lax.fori_loop(0, (n_long + MERGED - 1) // MERGED, list_block, 0)

        return 0

    @pl.when(chunk == 0)
    def _():
        dense(0, (w0, c0))

    share = all_enc_ref.shape[0] // (8 * n_chunks * n_tile)

    def all_starts(i):
        find_starts(all_enc_ref, all_start_ref, [(chunk * n_tile + i) * share + j for j in range(share)], own_sub)

    def pair(p, _):
        i = 2 * p
        dense(i + 1, (w1, c1))
        all_starts(i)
        add(i, (w0, c0))
        dense(i + 2, (w0, c0))
        all_starts(i + 1)
        add(i + 1, (w1, c1))
        return 0

    lax.fori_loop(0, n_tile // 2, pair, 0)

    lax.fori_loop(0, n_tile, rest, 0)

    n_all = n_tile * n_tok

    def rep_window(b, _):
        rows = pl.ds(pl.multiple_of(b * WINDOW, WINDOW), WINDOW)
        one_hot_rows((slot_ref[rows, :] >> log2(n_all * LANES)) - chunk * WIDE, WIDE, hot)
        v_rep[rows, :] += jnp.dot(hot[...], v_ref[...], preferred_element_type=jnp.float32).astype(jnp.bfloat16)
        u_rep[rows, :] += jnp.dot(hot[...], u_ref[...], preferred_element_type=jnp.float32).astype(jnp.bfloat16)
        return 0

    lax.fori_loop(off_ref[chunk] // WINDOW, (off_ref[chunk + 1] + WINDOW - 1) // WINDOW, rep_window, 0)

    @pl.when(chunk == n_chunk - 1)
    def _():
        def rep_block(b, _):
            rows = pl.ds(pl.multiple_of(b * BLOCK, BLOCK), BLOCK)
            slot = slot_ref[rows, :]
            token = jnp.where(slot >= 0, (slot >> log2(LANES)) & (n_all - 1), -1)
            one_hot_rows(token, n_all, wx)
            both = jnp.dot(wx[...], wc_ref[...], preferred_element_type=jnp.float32)
            mine = lane_iota(BLOCK) == (slot & (LANES - 1))
            weight = jnp.sum(jnp.where(mine, both[:, :LANES], 0.0), axis=1, keepdims=True)
            coef = jnp.sum(jnp.where(mine, both[:, LANES:], 0.0), axis=1, keepdims=True)
            for part in range(n_all // LANES):
                cols = slice(part * LANES, (part + 1) * LANES)
                hit = token == lane_iota(BLOCK) + part * LANES
                wx[:, cols] = jnp.where(hit, weight, 0.0).astype(jnp.bfloat16)
                cx[:, cols] = jnp.where(hit, coef, 0.0).astype(jnp.bfloat16)
            v_cols, u_cols = vt.at[:, :BLOCK], ut.at[:, :BLOCK]
            v_cols[...] = v_rep[rows, :].T
            u_cols[...] = u_rep[rows, :].T

            def spend(i, _):
                cols = pl.ds(pl.multiple_of(i * n_tok, n_tok), n_tok)
                acc_y[i] += jnp.dot(v_cols[...], wx[:, cols], preferred_element_type=jnp.float32)
                acc_dx[i] += jnp.dot(u_cols[...], cx[:, cols], preferred_element_type=jnp.float32)
                return 0

            lax.fori_loop(0, n_tile, spend, 0)
            return 0

        lax.fori_loop(0, (off_ref[n_chunk] + BLOCK - 1) // BLOCK, rep_block, 0)
        for i in range(n_tile):
            pltpu.make_async_copy(acc_y.at[i], out_ref.at[i, 0], sem.at[0]).start()
            pltpu.make_async_copy(acc_dx.at[i], out_ref.at[i, 1], sem.at[0]).start()
        for i in range(n_tile):
            pltpu.make_async_copy(acc_y.at[i], out_ref.at[i, 0], sem.at[0]).wait()
            pltpu.make_async_copy(acc_dx.at[i], out_ref.at[i, 1], sem.at[0]).wait()


def combine(n_tile, own_rows, tab, offs, table_u, table_v, enc, wc, starts, slots, all_enc):
    block_rows, width = table_u.shape
    n_all = enc.shape[0]
    n_tok = n_all // n_tile
    n_sub = block_rows // SUB
    q_per = LANES // n_sub
    n_lane_tile = -(-MERGED // q_per)
    n_row = n_lane_tile * LANES
    f32, bf16 = jnp.float32, jnp.bfloat16
    whole = lambda shape: pl.BlockSpec(shape, lambda c, t, o: (0, 0), pipeline_mode=pl.Buffered(1))
    return pl.pallas_call(
        functools.partial(combine_kernel, n_tok, n_sub, block_rows // WIDE, own_rows // SUB),
        grid_spec=pltpu.PrefetchScalarGridSpec(
            num_scalar_prefetch=2,
            grid=(block_rows // WIDE,),
            in_specs=[
                pl.BlockSpec((WIDE, width), lambda c, t, o: (c, 0)),
                pl.BlockSpec((WIDE, width), lambda c, t, o: (c, 0)),
                whole(enc.shape),
                whole(wc.shape),
                whole(starts.shape),
                whole(slots.shape),
                whole(all_enc.shape),
            ],
            out_specs=(pl.BlockSpec(memory_space=pl.ANY), whole(all_enc.shape)),
            scratch_shapes=[pltpu.VMEM((n_tile * n_row, n_tok), f32)] * 3
            + [pltpu.VMEM((n_lane_tile, n_tok, LANES), f32)] * 3
            + [pltpu.VMEM((n_row, n_tok), f32)] * 3
            + [pltpu.VMEM((n_lane_tile, n_tok, LANES), f32)] * 3
            + [pltpu.VMEM((n_tile, width, n_tok), f32)] * 2
            + [pltpu.VMEM((width, WIDE), bf16)] * 2
            + [pltpu.VMEM((WIDE, n_tok), bf16)] * 6
            + [pltpu.VMEM((slots.shape[0], width), bf16)] * 2
            + [pltpu.VMEM((WINDOW, WIDE), bf16)]
            + [pltpu.VMEM((BLOCK, n_all), bf16)] * 2
            + [pltpu.SemaphoreType.DMA((1,))],
        ),
        out_shape=(jax.ShapeDtypeStruct((n_tile, 2, width, n_tok), f32), jax.ShapeDtypeStruct(all_enc.shape, jnp.int32)),
        compiler_params=pltpu.CompilerParams(vmem_limit_bytes=VMEM_BYTES),
        cost_estimate=pl.CostEstimate(flops=4 * n_all * block_rows * width, bytes_accessed=12 * n_all * width, transcendentals=0),
        name='combine',
    )(tab, offs, table_u, table_v, enc, wc, starts, slots, all_enc)


def grad_kernel(n_sub, tab_ref, off_ref, x_ref, dy_ref, enc_ref, wc_ref, start_ref, slot_ref, place_ref, du_ref, dv_ref,
                le, lw, lc, te, tw, tc, se, sw, sc, re, rw, rc, acc_u, acc_v, w0, c0, w1, c1, w2, c2,
                x_rep, dy_rep, w_rep, c_rep, hot):
    step = pl.program_id(0)
    n_step = pl.num_programs(0)
    n_tok = x_ref.shape[0]
    lists, tmps, spare, spare_tmps = (le, lw, lc), (te, tw, tc), (se, sw, sc), (re, rw, rc)
    per = WIDE // SUB
    own_rows = acc_u.shape[0]
    n_chunk = own_rows // WIDE
    bufs = ((w0, c0), (w1, c1))
    n_group = n_tok // 8

    @pl.when(step == 0)
    def _():
        acc_u[...] = jnp.zeros_like(acc_u)
        acc_v[...] = jnp.zeros_like(acc_v)
        for ref in (x_rep, dy_rep, w_rep, c_rep):
            ref[...] = jnp.zeros_like(ref)
        expand_groups(enc_ref, wc_ref, start_ref, 0, range(n_group), n_sub, 0, tmps)

    def add(k, pair):
        rows = slice(k * WIDE, (k + 1) * WIDE) if isinstance(k, int) else pl.ds(pl.multiple_of(k * WIDE, WIDE), WIDE)
        acc_v[rows, :] += jnp.dot(pair[0][:, :n_tok], dy_ref[...], preferred_element_type=jnp.float32)
        acc_u[rows, :] += jnp.dot(pair[1][:, :n_tok], x_ref[...], preferred_element_type=jnp.float32)

    turn_lists(tmps, lists, 0)
    next_tok = jnp.minimum(step + 1, n_step - 1) * n_tok
    densify(lists, 0, 0, n_sub, 0, bufs[0])
    for k in range(n_chunk):
        if k + 1 < n_chunk:
            densify(lists, 0, (k + 1) * per, n_sub, 0, bufs[(k + 1) % 2])
        expand_groups(enc_ref, wc_ref, start_ref, next_tok, range(k * n_group // n_chunk, (k + 1) * n_group // n_chunk), n_sub, 0, tmps)
        add(k, bufs[k % 2])

    n_layer, n_long = tab_ref[0, step], tab_ref[1, step]

    @pl.when((n_layer > 1) | (n_long > MERGED))
    def _():
        def list_block(qb, _):
            expand_slowly(enc_ref, wc_ref, start_ref, step * n_tok, n_tok, n_sub, qb * MERGED, spare_tmps, spare)

            def rest(k, _):
                def layer_step(r, _):
                    densify(spare, 0, k * per, n_sub, r, (w2, c2))
                    add(k, (w2, c2))
                    return 0

                lax.fori_loop(jnp.where(qb == 0, 1, 0), n_layer, layer_step, 0)
                return 0

            lax.fori_loop(0, n_chunk, rest, 0)
            return 0

        lax.fori_loop(0, (n_long + MERGED - 1) // MERGED, list_block, 0)

    def rep_window(b, _):
        rows = pl.ds(pl.multiple_of(b * WINDOW, WINDOW), WINDOW)
        slot = slot_ref[rows, :]
        one_hot_rows(jnp.where(slot >= 0, (slot >> log2(own_rows * LANES)) - step * n_tok, -1), n_tok, hot)
        x_rep[rows, :] += jnp.dot(hot[...], x_ref[...], preferred_element_type=jnp.float32).astype(jnp.bfloat16)
        dy_rep[rows, :] += jnp.dot(hot[...], dy_ref[...], preferred_element_type=jnp.float32).astype(jnp.bfloat16)
        both = jnp.dot(hot[...], wc_ref[pl.ds(pl.multiple_of(step * n_tok, n_tok), n_tok), :], preferred_element_type=jnp.float32)
        mine = lane_iota(WINDOW) == (slot & (LANES - 1))
        weight = jnp.sum(jnp.where(mine, both[:, :LANES], 0.0), axis=1, keepdims=True)
        coef = jnp.sum(jnp.where(mine, both[:, LANES:], 0.0), axis=1, keepdims=True)
        w_rep[rows, :] += jnp.broadcast_to(weight, (WINDOW, LANES))
        c_rep[rows, :] += jnp.broadcast_to(coef, (WINDOW, LANES))
        return 0

    lax.fori_loop(off_ref[step] // WINDOW, (off_ref[step + 1] + WINDOW - 1) // WINDOW, rep_window, 0)

    @pl.when(step == pl.num_programs(0) - 1)
    def _():
        def rep_block(b, _):
            rows = pl.ds(pl.multiple_of(b * BLOCK, BLOCK), BLOCK)
            place = place_ref[0:1, rows].astype(jnp.float32)
            weight = w_rep[rows, :].T[0:1, :]
            coef = c_rep[rows, :].T[0:1, :]

            def spend(k, _):
                for part in range(per):
                    shift = (k * WIDE + part * SUB).astype(jnp.float32)
                    fill_tile([(place - shift, weight, coef)], BLOCK, part, (w2, c2))
                own = pl.ds(pl.multiple_of(k * WIDE, WIDE), WIDE)
                acc_v[own, :] += jnp.dot(w2[:, :BLOCK], dy_rep[rows, :], preferred_element_type=jnp.float32)
                acc_u[own, :] += jnp.dot(c2[:, :BLOCK], x_rep[rows, :], preferred_element_type=jnp.float32)
                return 0

            lax.fori_loop(0, n_chunk, spend, 0)
            return 0

        lax.fori_loop(0, (off_ref[pl.num_programs(0)] + BLOCK - 1) // BLOCK, rep_block, 0)
        du_ref[...] = acc_u[...].astype(jnp.bfloat16)
        dv_ref[...] = acc_v[...].astype(jnp.bfloat16)


def table_grads(own_rows, tab, offs, tok_pair, enc, wc, starts, slots, places):
    n_all, pair_width = tok_pair.shape
    width = pair_width // 2
    tile = min(512, n_all)
    n_sub = own_rows // SUB
    q_per = LANES // n_sub
    n_lane_tile = -(-MERGED // q_per)
    n_row = n_lane_tile * LANES
    f32, bf16 = jnp.float32, jnp.bfloat16
    out = jax.ShapeDtypeStruct((own_rows, width), bf16)
    whole = lambda shape: pl.BlockSpec(shape, lambda s, t, o: (0, 0), pipeline_mode=pl.Buffered(1))
    return pl.pallas_call(
        functools.partial(grad_kernel, n_sub),
        grid_spec=pltpu.PrefetchScalarGridSpec(
            num_scalar_prefetch=2,
            grid=(n_all // tile,),
            in_specs=[
                pl.BlockSpec((tile, width), lambda s, t, o: (s, 0)),
                pl.BlockSpec((tile, width), lambda s, t, o: (s, 1)),
                whole(enc.shape),
                whole(wc.shape),
                whole(starts.shape),
                whole(slots.shape),
                whole(places.shape),
            ],
            out_specs=[whole((own_rows, width))] * 2,
            scratch_shapes=([pltpu.VMEM((n_row, tile), f32)] * 3 + [pltpu.VMEM((n_lane_tile, tile, LANES), f32)] * 3) * 2
            + [pltpu.VMEM((own_rows, width), f32)] * 2
            + [pltpu.VMEM((WIDE, tile), bf16)] * 4
            + [pltpu.VMEM((WIDE, max(tile, BLOCK)), bf16)] * 2
            + [pltpu.VMEM((slots.shape[0], width), bf16)] * 2
            + [pltpu.VMEM((slots.shape[0], LANES), f32)] * 2
            + [pltpu.VMEM((WINDOW, tile), bf16)],
        ),
        out_shape=(out, out),
        compiler_params=pltpu.CompilerParams(vmem_limit_bytes=VMEM_BYTES),
        cost_estimate=pl.CostEstimate(flops=4 * n_all * own_rows * width, bytes_accessed=4 * n_all * width, transcendentals=0),
        name='table_grads',
    )(tab, offs, tok_pair, tok_pair, enc, wc, starts, slots, places)


def repeat_slots(inside, key, major_of, bounds, n_slot):
    n_in = jnp.sum(inside.astype(jnp.int32))
    slots = lax.sort(jnp.where(inside, key, BIG).reshape(-1))[:n_slot]
    slots = jnp.where(jnp.arange(n_slot, dtype=jnp.int32) < n_in, slots, -1)
    major = jnp.where(slots >= 0, slots // major_of, BIG)
    offs = jnp.sum((major[None, :] < bounds[:, None]).astype(jnp.int32), axis=1)
    return slots, offs, n_in


def solution(mesh):
    owners = mesh.shape['table']
    copies = mesh.shape['data']
    tok_spec = P(('rep', 'data', 'table'), None)
    sel_spec = P(('rep', 'data', 'table'), None, None)
    row_spec = P(('rep', 'table'), None)
    grad_spec = P(('rep', 'table', 'data'), None)

    def device_fn(tokens, table_u, table_v, expert_ids, gate_vals, grad_out):
        n_tok, _ = tokens.shape
        sel = expert_ids.shape[1] * expert_ids.shape[2]
        block_rows = table_u.shape[0]
        own_rows = block_rows // copies
        my_block = lax.axis_index('table')
        my_copy = lax.axis_index('data')

        ids_sorted, gates = lax.sort((expert_ids.reshape(n_tok, sel), gate_vals.reshape(n_tok, sel)), dimension=1, num_keys=1)
        enc, tab, rep_key = prepare(ids_sorted)
        n_place = n_tok * sel
        n_rep = REP_ROWS * LANES
        rep_key = lax.sort(rep_key[:, :REP_TOKEN].reshape(-1))[:n_rep]
        is_rep = jnp.arange(n_rep, dtype=jnp.int32) < tab[2, 0].astype(jnp.int32)
        rep_id = jnp.where(is_rep, rep_key >> log2(n_place), -1).astype(jnp.float32).reshape(REP_ROWS, LANES)
        rep_pos = (rep_key & (n_place - 1)).astype(jnp.float32).reshape(REP_ROWS, LANES)
        lists = jnp.concatenate([enc, tab, rep_id, rep_pos], axis=0)
        n_extra = lists.shape[0] - n_tok
        lists_gates = jnp.concatenate([lists, jnp.concatenate([gates, jnp.zeros((n_extra, sel), jnp.float32)], axis=0)], axis=1)
        pair = jnp.concatenate([tokens, grad_out], axis=1)

        row_q = lax.all_gather(lists_gates, 'table', axis=0, tiled=False)
        row_pair = lax.all_gather(pair, 'table', axis=0, tiled=True)
        row_enc = row_q[:, :n_tok, :sel].reshape(owners * n_tok, sel).astype(jnp.int32) - my_block * (block_rows * LANES)
        row_gate = row_q[:, :n_tok, sel:].reshape(owners * n_tok, sel)
        n_chunk = block_rows // WIDE

        def limits(got, over, per_step):
            most = got[:, n_tok:n_tok + 2, 0].reshape(-1, per_step, 2).max(axis=1).astype(jnp.int32) + 1
            return jnp.where(over, most, 1).T

        def repeats(got):
            extra = got[:, n_tok + tab.shape[0]:].astype(jnp.int32).reshape(got.shape[0], 2, n_rep)
            over = jnp.any((got[:, n_tok + 2, 0] > n_rep) | (got[:, n_tok + 3, 0] > REP_TOKEN))
            token = jnp.arange(got.shape[0], dtype=jnp.int32)[:, None] * n_tok + extra[:, 1] // sel
            return extra[:, 0], token, extra[:, 1] & (sel - 1), over

        row_all = owners * n_tok
        rep_ids, rep_tok, rep_lane, over = repeats(row_q[:, :, :sel])
        rep_row = rep_ids - my_block * block_rows
        inside = (rep_ids >= 0) & (rep_row >= 0) & (rep_row < block_rows)
        bounds = jnp.arange(n_chunk + 1, dtype=jnp.int32) * WIDE
        n_slot = -(-row_all * 5 // (8 * BLOCK)) * BLOCK
        row_slots, row_offs, n_in = repeat_slots(inside, (rep_row * row_all + rep_tok) * sel + rep_lane, row_all * sel, bounds, n_slot)
        over = over | (n_in > n_slot)
        row_tab = limits(row_q, over, 1)
        row_offs = jnp.where(over, 0, row_offs)
        row_slots = jnp.broadcast_to(row_slots[:, None], (n_slot, LANES))

        late_pair, late_lists, row_pair = lax.optimization_barrier((pair, lists, row_pair))
        all_lists = lax.all_gather(late_lists, ('data', 'table'), axis=0, tiled=False)
        all_pair = lax.all_gather(late_pair, ('data', 'table'), axis=0, tiled=True)

        wc, row_starts = scores(row_pair, table_u, table_v, row_enc, row_gate)
        all_wc = lax.all_gather(wc, 'data', axis=0, tiled=True)
        first_row = my_block * block_rows + my_copy * own_rows
        all_enc = all_lists[:, :n_tok, :].reshape(-1, sel).astype(jnp.int32) - first_row * LANES
        part, all_starts = combine(owners, own_rows, row_tab, row_offs, table_u, table_v, row_enc, wc, row_starts, row_slots, all_enc)
        own = lax.psum_scatter(part, 'table', scatter_dimension=0, tiled=True)[0]

        tile = min(512, owners * copies * n_tok)
        rep_ids, rep_tok, rep_lane, over = repeats(all_lists)
        rep_row = rep_ids - first_row
        inside = (rep_ids >= 0) & (rep_row >= 0) & (rep_row < own_rows)
        n_all = owners * copies * n_tok
        bounds = jnp.arange(n_all // tile + 1, dtype=jnp.int32) * tile
        n_slot = -(-n_all * 5 // (32 * BLOCK)) * BLOCK
        all_slots, all_offs, n_in = repeat_slots(inside, (rep_tok * own_rows + rep_row) * sel + rep_lane, own_rows * sel, bounds, n_slot)
        over = over | (n_in > n_slot)
        all_tab = limits(all_lists, over, tile // n_tok)
        all_offs = jnp.where(over, 0, all_offs)
        places = jnp.where(all_slots >= 0, (all_slots // sel) & (own_rows - 1), -1)
        places = jnp.broadcast_to(places[None, :], (8, n_slot))
        all_slots = jnp.broadcast_to(all_slots[:, None], (n_slot, LANES))
        grad_u, grad_v = table_grads(own_rows, all_tab, all_offs, all_pair, all_enc, all_wc, all_starts, all_slots, places)
        return own[0].T.astype(jnp.bfloat16), own[1].T.astype(jnp.bfloat16), grad_u, grad_v

    return jax.shard_map(device_fn, mesh=mesh, in_specs=(tok_spec, row_spec, row_spec, sel_spec, sel_spec, tok_spec), out_specs=(tok_spec, tok_spec, grad_spec, grad_spec), check_vma=False)
```
